256 devices in a mesh: feat: 8 (over z_hi, core), tok: 32 (over y, z_lo, x).
Axes of the slice: x: 4, y: 4, z: 8 (z_hi: 4, z_lo: 2; z = z_hi * 2 + z_lo), core: 2. Of those that a mesh axis runs over, the one named last changes fastest.
Arguments:
- activations: bfloat16 [8192, 28672], P('tok', 'feat'), may hold values from -160 to 160
- dense_rows: float32 [64, 28672], P(None, 'feat'), may hold values from -6 to 6
- targets: float32 [8192, 64], P('tok'), may hold values from -6 to 6
Outputs:
- pruned_rows: float32 [64, 28672], P(None, 'feat')
The draws below stay inside these ranges and needn't reach their ends.
All inputs are finite; a program needn't handle non-finite values.
Results may differ from the reference program's by a relative error of at most 0.0055.
Values may be sent and summed in bfloat16 or wider, within the bound.
A program may use at most 64 MiB of HBM per device.

```python
import math
import jax
import jax.numpy as jnp
from jax import lax

DIN = 28672
ROWS = 64
ITERS = 4
TOKENS = 8192


def draw_activations(key, part):
    key_cols = jax.random.fold_in(key, 11)
    key_vals = jax.random.fold_in(key, 12)
    position = jnp.arange(DIN, dtype=jnp.float32) / DIN
    spread = jnp.exp(jax.random.uniform(key_cols, (DIN,), jnp.float32, math.log(0.3), math.log(3.0)))
    values = jax.random.truncated_normal(key_vals, -4.0, 4.0, (TOKENS, DIN), jnp.float32)
    column_scale = spread * jnp.power(3.0, position)
    return (values * column_scale[None, :]).astype(jnp.bfloat16)


def block_levels(rng, dims, shards, smallest, high):
    def one(dim, parts):
        heights = jax.random.uniform(jax.random.fold_in(jax.random.fold_in(rng, 6), dim), (parts,), jnp.float32, smallest / len(shards), high / len(shards))
        return jnp.repeat(jnp.exp(heights), dims[dim] // parts).reshape((-1,) + (1,) * (len(dims) - dim - 1))

    loudness = one(*shards[0])
    for cut in shards[1:]:
        loudness = loudness * one(*cut)
    return loudness


def normal_values(stream_key, dims, deviation, limit, split=(), held_as=jnp.bfloat16):
    drawn = deviation * jax.random.normal(stream_key, dims, jnp.float32)
    if split:
        drawn = drawn * block_levels(stream_key, dims, split, -0.22, 0.18)
    return jnp.clip(drawn, -limit, limit).astype(held_as)


def setup_inputs(seed: int = 0) -> dict:
    key_of = jax.random.split(jax.random.key(seed), 4)
    return {
        "activations": draw_activations(jax.random.fold_in(key_of[3], 71), 0),
        "dense_rows": normal_values(key_of[1], (ROWS, DIN), 1.0, 6.0, ((1, 8),), jnp.float32),
        "targets": normal_values(key_of[2], (TOKENS, ROWS), 1.0, 6.0, ((0, 32),), jnp.float32),
    }


step_size = 0.25
threshold = 0.2
epsilon = 1e-06

def momentum_terms(iterations):
    values = []
    current = 1.0
    for _ in range(iterations):
        upcoming = (1.0 + math.sqrt(1.0 + 4.0 * current * current)) / 2.0
        values.append((current - 1.0) / upcoming)
        current = upcoming
    return values

def reference(activations, dense_rows, targets):
    factor = DIN ** (-0.5)
    momentum = momentum_terms(ITERS)
    weights = dense_rows
    advance = dense_rows
    for iteration in range(ITERS):
        rounded = advance.astype(jnp.bfloat16)
        summed = lax.dot_general(activations, rounded, (((1,), (1,)), ((), ())), preferred_element_type=jnp.float32)
        residual = (factor * summed - targets).astype(jnp.bfloat16)
        gradient = lax.dot_general(residual, activations, (((0,), (0,)), ((), ())), preferred_element_type=jnp.float32)
        mean_square = jnp.sum(gradient * gradient) / (ROWS * DIN)
        moved = advance - step_size * gradient * lax.rsqrt(mean_square + epsilon)
        shrunk = jnp.sign(moved) * jnp.maximum(jnp.abs(moved) - threshold, 0.0)
        advance = shrunk + momentum[iteration] * (shrunk - weights)
        weights = shrunk
    return weights
```

```python
import math

import jax
import jax.numpy as jnp
from jax import lax
from jax.experimental import pallas as pl
from jax.experimental.pallas import tpu as pltpu
from jax.sharding import PartitionSpec as P

DIN = 28672
ROWS = 64
ITERS = 4

step_size = 0.25
threshold = 0.2
epsilon = 1e-06

MESH = pl.DeviceIdType.MESH
FEAT = 8
TOK = 32
TOKENS = 256
HALF = TOKENS // 2
COLS = DIN // FEAT
PIECE_ROWS = 8
PIECE_COLS = COLS // 4


def momentum_terms(iterations):
    values = []
    current = 1.0
    for _ in range(iterations):
        upcoming = (1.0 + math.sqrt(1.0 + 4.0 * current * current)) / 2.0
        values.append((current - 1.0) / upcoming)
        current = upcoming
    return values


OFFSETS = sorted(
    [(dy, dz, dx) for dy in range(4) for dz in range(2) for dx in range(4) if (dy, dz, dx) != (0, 0, 0)],
    key=lambda o: -(min(o[0], 4 - o[0]) + o[1] + min(o[2], 4 - o[2])),
)


def kernel(
    act_hbm, dense_hbm, targets_ref, out_ref,
    act, ahead, low, goal,
    partial, pair_in, half_out, half_in, residual,
    pieces, arrived, gathered, square_feat, square_tok, square_part,
    load_sem, sem,
):
    feat = lax.axis_index("feat")
    tok = lax.axis_index("tok")
    core = lax.rem(feat, 2)
    partner = feat + 1 - 2 * core
    y, z, x = tok // 8, lax.rem(tok // 4, 2), lax.rem(tok, 4)

    def tok_at(offset):
        dy, dz, dx = offset
        return lax.rem(y + dy, 4) * 8 + lax.rem(z + dz, 2) * 4 + lax.rem(x + dx, 4)

    barrier = pltpu.get_barrier_semaphore()
    for offset in OFFSETS:
        pl.semaphore_signal(barrier, inc=1, device_id={"tok": tok_at(offset)}, device_id_type=MESH)
    for k in range(1, FEAT):
        pl.semaphore_signal(barrier, inc=1, device_id={"feat": lax.rem(feat + k, FEAT)}, device_id_type=MESH)

    load_dense = pltpu.make_async_copy(dense_hbm, ahead, load_sem.at[0])
    load_act = pltpu.make_async_copy(act_hbm, act, load_sem.at[1])
    load_dense.start()
    load_act.start()
    goal[...] = targets_ref[pl.ds(pl.multiple_of(core * HALF, HALF), HALF), :].T
    load_dense.wait()
    out_ref[...] = ahead[...]
    low[...] = ahead[...].astype(jnp.bfloat16)
    load_act.wait()
    pl.semaphore_wait(barrier, TOK + FEAT - 2)

    momentum = momentum_terms(ITERS)
    factor = DIN ** (-0.5)

    def copy_to(src, dst, send, recv, device):
        copy = pltpu.make_async_remote_copy(
            src_ref=src, dst_ref=dst, send_sem=send, recv_sem=recv, device_id=device, device_id_type=MESH
        )
        copy.start()

    def wait_for(ref, semaphore):
        pltpu.make_async_copy(ref, ref, semaphore).wait()

    def iteration(it, _):
        def s(i):
            return sem.at[it, i]

        product = lax.dot_general(
            low[...], act[...], (((1,), (1,)), ((), ())), preferred_element_type=jnp.float32
        )
        partial[it, 0] = product[:, :HALF]
        partial[it, 1] = product[:, HALF:]
        copy_to(partial.at[it, 1 - core], pair_in.at[it], s(0), s(1), {"feat": partner})
        wait_for(pair_in.at[it], s(1))
        half = partial[it, core] + pair_in[it]
        half_out[it] = half.astype(jnp.bfloat16)
        for k in (2, 1, 3):
            copy_to(half_out.at[it], half_in.at[it, k - 1], s(2), s(3), {"feat": lax.rem(feat + 2 * k, FEAT)})
        wait_for(half_in.at[it], s(3))
        for k in range(3):
            half = half + half_in[it, k].astype(jnp.float32)
        residual[it, core] = (factor * half - goal[...]).astype(jnp.bfloat16)
        copy_to(residual.at[it, core], residual.at[it, core], s(4), s(5), {"feat": partner})
        wait_for(residual.at[it, 1 - core], s(5))
        whole = jnp.concatenate([residual[it, 0], residual[it, 1]], axis=1)

        for dx in (2, 3, 0, 1):
            cx = lax.rem(x + dx, 4)
            columns = pl.ds(pl.multiple_of(cx * PIECE_COLS, 128), PIECE_COLS)
            block = jnp.dot(whole, act[:, columns], preferred_element_type=jnp.float32)
            for g in range(8):
                pieces[it, g * 4 + cx] = block[g * 8 : g * 8 + 8].astype(jnp.bfloat16)
            for offset in OFFSETS:
                if offset[2] == dx:
                    to = tok_at(offset)
                    copy_to(pieces.at[it, to], arrived.at[it, tok], s(6), s(7), {"tok": to})
        arrived[it, tok] = pieces[it, tok]
        wait_for(arrived.at[it, pl.ds(0, TOK - 1)], s(7))

        total = arrived[it, 0].astype(jnp.float32)
        for p in range(1, TOK):
            total = total + arrived[it, p].astype(jnp.float32)
        gathered[it, tok] = total.astype(jnp.bfloat16)
        square = total * total
        lanes = square[:, :128]
        for c in range(1, PIECE_COLS // 128):
            lanes = lanes + square[:, c * 128 : c * 128 + 128]
        square_feat[it, feat] = jnp.sum(lanes, axis=0, keepdims=True)
        for k in range(1, FEAT):
            copy_to(
                square_feat.at[it, feat], square_feat.at[it, feat], s(8), s(9), {"feat": lax.rem(feat + k, FEAT)}
            )
        for offset in OFFSETS:
            copy_to(gathered.at[it, tok], gathered.at[it, tok], s(10), s(11), {"tok": tok_at(offset)})

        wait_for(square_feat.at[it, pl.ds(0, FEAT - 1)], s(9))
        square_tok[it, tok] = jnp.sum(square_feat[it], axis=0)
        for offset in OFFSETS:
            copy_to(square_tok.at[it, tok], square_tok.at[it, tok], s(12), s(13), {"tok": tok_at(offset)})
        wait_for(square_tok.at[it, pl.ds(0, TOK - 1)], s(13))
        wait_for(gathered.at[it, pl.ds(0, TOK - 1)], s(11))

        total_square = jnp.sum(jnp.sum(square_tok[it], axis=0), axis=1, keepdims=True)
        scale = step_size * lax.rsqrt(total_square / (ROWS * DIN) + epsilon)
        m = jnp.float32(momentum[0])
        for i in range(1, ITERS):
            m = jnp.where(it == i, jnp.float32(momentum[i]), m)

        for c in range(4):
            columns = slice(c * PIECE_COLS, (c + 1) * PIECE_COLS)
            for r in range(4):
                rows = slice(r * 16, r * 16 + 16)
                gradient = jnp.concatenate(
                    [gathered[it, 8 * r + c].astype(jnp.float32), gathered[it, 8 * r + 4 + c].astype(jnp.float32)],
                    axis=0,
                )
                moved = ahead[rows, columns] - scale * gradient
                shrunk = moved - jnp.clip(moved, -threshold, threshold)
                advance = shrunk + m * (shrunk - out_ref[rows, columns])
                out_ref[rows, columns] = shrunk
                ahead[rows, columns] = advance
                low[rows, columns] = advance.astype(jnp.bfloat16)

        wait_for(partial.at[it, 0], s(0))
        wait_for(half_in.at[it], s(2))
        wait_for(residual.at[it, 0], s(4))
        wait_for(arrived.at[it, pl.ds(0, TOK - 1)], s(6))
        wait_for(square_feat.at[it, pl.ds(0, FEAT - 1)], s(8))
        wait_for(gathered.at[it, pl.ds(0, TOK - 1)], s(10))
        wait_for(square_tok.at[it, pl.ds(0, TOK - 1)], s(12))
        return 0

    lax.fori_loop(0, ITERS, iteration, 0)


def shards(activations, dense_rows, targets):
    bf16, f32 = jnp.bfloat16, jnp.float32
    return pl.pallas_call(
        kernel,
        out_shape=jax.ShapeDtypeStruct((ROWS, COLS), f32),
        in_specs=[
            pl.BlockSpec(memory_space=pl.ANY),
            pl.BlockSpec(memory_space=pl.ANY),
            pl.BlockSpec(memory_space=pltpu.VMEM),
        ],
        out_specs=pl.BlockSpec(memory_space=pltpu.VMEM),
        scratch_shapes=[
            pltpu.VMEM((TOKENS, COLS), bf16),
            pltpu.VMEM((ROWS, COLS), f32),
            pltpu.VMEM((ROWS, COLS), bf16),
            pltpu.VMEM((ROWS, HALF), f32),
            pltpu.VMEM((ITERS, 2, ROWS, HALF), f32),
            pltpu.VMEM((ITERS, ROWS, HALF), f32),
            pltpu.VMEM((ITERS, ROWS, HALF), bf16),
            pltpu.VMEM((ITERS, 3, ROWS, HALF), bf16),
            pltpu.VMEM((ITERS, 2, ROWS, HALF), bf16),
            pltpu.VMEM((ITERS, TOK, PIECE_ROWS, PIECE_COLS), bf16),
            pltpu.VMEM((ITERS, TOK, PIECE_ROWS, PIECE_COLS), bf16),
            pltpu.VMEM((ITERS, TOK, PIECE_ROWS, PIECE_COLS), bf16),
            pltpu.VMEM((ITERS, FEAT, 1, 128), f32),
            pltpu.VMEM((ITERS, TOK, 1, 128), f32),
            pltpu.VMEM((1, 128), f32),
            pltpu.SemaphoreType.DMA((2,)),
            pltpu.SemaphoreType.DMA((ITERS, 14)),
        ],
        compiler_params=pltpu.CompilerParams(collective_id=0, has_side_effects=True),
    )(activations, dense_rows, targets)


def solution(mesh):
    in_specs = (P("tok", "feat"), P(None, "feat"), P("tok", None))
    out_specs = P(None, "feat")
    return jax.shard_map(shards, mesh=mesh, in_specs=in_specs, out_specs=out_specs, check_vma=False)
```

```python
import math

import jax
import jax.numpy as jnp
from jax import lax
from jax.experimental import pallas as pl
from jax.experimental.pallas import tpu as pltpu
from jax.sharding import PartitionSpec as P

DIN = 28672
ROWS = 64
ITERS = 4

step_size = 0.25
threshold = 0.2
epsilon = 1e-06

MESH = pl.DeviceIdType.MESH
FEAT = 8
TOK = 32
TOKENS = 256
HALF = TOKENS // 2
COLS = DIN // FEAT
PIECE_ROWS = 8
PIECE_COLS = COLS // 4


def momentum_terms(iterations):
    values = []
    current = 1.0
    for _ in range(iterations):
        upcoming = (1.0 + math.sqrt(1.0 + 4.0 * current * current)) / 2.0
        values.append((current - 1.0) / upcoming)
        current = upcoming
    return values


def ring(offset, size):
    return min(offset, size - offset)


TOKEN_PEERS = sorted(
    [(dy, dz, dx) for dy in range(4) for dz in range(2) for dx in range(4) if (dy, dz, dx) != (0, 0, 0)],
    key=lambda o: -(ring(o[0], 4) + o[1] + ring(o[2], 4)),
)
LINE_PEERS = sorted(
    [(dz, dc) for dz in range(8) for dc in range(2) if (dz, dc) != (0, 0)], key=lambda o: -ring(o[0], 8) - o[1] / 2
)
PLANE_PEERS = sorted(
    [(dy, dx) for dy in range(4) for dx in range(4) if (dy, dx) != (0, 0)],
    key=lambda o: -(ring(o[0], 4) + ring(o[1], 4)),
)


def kernel(
    act_hbm, dense_hbm, targets_hbm, weights,
    act, ahead, low, targets,
    partial, pair_in, half_out, half_in, residual,
    pieces, arrived, gathered, line_squares, plane_squares,
    load_sem, sem,
):
    load_dense = pltpu.make_async_copy(dense_hbm, ahead, load_sem.at[0])
    load_act = pltpu.make_async_copy(act_hbm, act, load_sem.at[1])
    load_targets = pltpu.make_async_copy(targets_hbm, targets, load_sem.at[2])
    load_dense.start()
    load_act.start()
    load_targets.start()

    feat = lax.axis_index("feat")
    tok = lax.axis_index("tok")
    core = lax.rem(feat, 2)
    partner = feat + 1 - 2 * core
    y, z_lo, x = tok // 8, lax.rem(tok // 4, 2), lax.rem(tok, 4)
    z = (feat // 2) * 2 + z_lo

    def token_peer(offset):
        dy, dz, dx = offset
        return lax.rem(y + dy, 4) * 8 + lax.rem(z_lo + dz, 2) * 4 + lax.rem(x + dx, 4)

    def line_peer(offset):
        dz, dc = offset
        to = lax.rem(z + dz, 8)
        return {"feat": (to // 2) * 2 + lax.rem(core + dc, 2), "tok": y * 8 + lax.rem(to, 2) * 4 + x}

    barrier = pltpu.get_barrier_semaphore()
    for offset in TOKEN_PEERS:
        pl.semaphore_signal(barrier, inc=1, device_id={"tok": token_peer(offset)}, device_id_type=MESH)
    for k in range(1, FEAT):
        pl.semaphore_signal(barrier, inc=1, device_id={"feat": lax.rem(feat + k, FEAT)}, device_id_type=MESH)

    def predict(it):
        product = lax.dot_general(
            low[...], act[...], (((1,), (1,)), ((), ())), preferred_element_type=jnp.float32
        )
        partial[it, 0] = product[:, :HALF]
        partial[it, 1] = product[:, HALF:]

    load_dense.wait()
    weights[...] = ahead[...]
    low[...] = ahead[...].astype(jnp.bfloat16)
    load_act.wait()
    load_targets.wait()
    predict(0)
    pl.semaphore_wait(barrier, TOK + FEAT - 2)

    momentum = momentum_terms(ITERS)
    factor = DIN ** (-0.5)

    def copy_to(src, dst, send, recv, device):
        pltpu.make_async_remote_copy(
            src_ref=src, dst_ref=dst, send_sem=send, recv_sem=recv, device_id=device, device_id_type=MESH
        ).start()

    def wait_for(ref, semaphore):
        pltpu.make_async_copy(ref, ref, semaphore).wait()

    def iteration(it, _):
        def s(i):
            return sem.at[it, i]

        copy_to(partial.at[it, 1 - core], pair_in.at[it], s(0), s(1), {"feat": partner})
        wait_for(pair_in.at[it], s(1))
        half = partial[it, core] + pair_in[it]
        half_out[it] = half.astype(jnp.bfloat16)
        for k in (2, 1, 3):
            copy_to(half_out.at[it], half_in.at[it, k - 1], s(2), s(3), {"feat": lax.rem(feat + 2 * k, FEAT)})
        goal = targets[:, pl.ds(pl.multiple_of(core * HALF, HALF), HALF)]
        wait_for(half_in.at[it], s(3))
        for k in range(3):
            half = half + half_in[it, k].astype(jnp.float32)
        residual[it, core] = (factor * half - goal).astype(jnp.bfloat16)
        copy_to(residual.at[it, core], residual.at[it, core], s(4), s(5), {"feat": partner})
        wait_for(residual.at[it, 1 - core], s(5))
        whole = jnp.concatenate([residual[it, 0], residual[it, 1]], axis=1)

        for dx in (2, 3, 0, 1):
            cx = lax.rem(x + dx, 4)
            columns = pl.ds(pl.multiple_of(cx * PIECE_COLS, 128), PIECE_COLS)
            block = jnp.dot(whole, act[:, columns], preferred_element_type=jnp.float32)
            for g in range(8):
                pieces[it, g * 4 + cx] = block[g * 8 : g * 8 + 8].astype(jnp.bfloat16)
            for offset in TOKEN_PEERS:
                if offset[2] == dx:
                    to = token_peer(offset)
                    copy_to(pieces.at[it, to], arrived.at[it, tok], s(6), s(7), {"tok": to})
        arrived[it, tok] = pieces[it, tok]
        wait_for(arrived.at[it, pl.ds(0, TOK - 1)], s(7))
        total = arrived[it, 0].astype(jnp.float32)
        for p in range(1, TOK):
            total = total + arrived[it, p].astype(jnp.float32)
        gathered[it, tok] = total.astype(jnp.bfloat16)
        square = total * total
        lanes = square[:, :128]
        for c in range(1, PIECE_COLS // 128):
            lanes = lanes + square[:, c * 128 : c * 128 + 128]

        def spread(squares, slot, value, send, recv, devices):
            squares[it, slot] = value
            for device in devices:
                copy_to(squares.at[it, slot], squares.at[it, slot], send, recv, device)

        def collected(squares, recv):
            wait_for(squares.at[it, pl.ds(0, 15)], recv)
            sums = [squares[it, p] for p in range(16)]
            while len(sums) > 1:
                sums = [a + b for a, b in zip(sums[::2], sums[1::2])]
            return sums[0]

        spread(
            line_squares, z * 2 + core, jnp.sum(lanes, axis=0, keepdims=True), s(8), s(9),
            [line_peer(offset) for offset in LINE_PEERS],
        )
        for offset in TOKEN_PEERS:
            copy_to(gathered.at[it, tok], gathered.at[it, tok], s(10), s(11), {"tok": token_peer(offset)})
        spread(
            plane_squares, y * 4 + x, collected(line_squares, s(9)), s(12), s(13),
            [{"tok": token_peer((dy, 0, dx))} for dy, dx in PLANE_PEERS],
        )
        total_square = jnp.sum(collected(plane_squares, s(13)), axis=1, keepdims=True)
        scale = step_size * lax.rsqrt(total_square / (ROWS * DIN) + epsilon)
        m = jnp.float32(momentum[0])
        for i in range(1, ITERS):
            m = jnp.where(it == i, jnp.float32(momentum[i]), m)

        wait_for(gathered.at[it, pl.ds(0, TOK - 1)], s(11))
        for c in range(4):
            columns = slice(c * PIECE_COLS, (c + 1) * PIECE_COLS)
            for r in range(4):
                rows = slice(r * 16, r * 16 + 16)
                gradient = jnp.concatenate(
                    [gathered[it, 8 * r + c].astype(jnp.float32), gathered[it, 8 * r + 4 + c].astype(jnp.float32)],
                    axis=0,
                )
                moved = ahead[rows, columns] - scale * gradient
                shrunk = moved - jnp.clip(moved, -threshold, threshold)
                advance = shrunk + m * (shrunk - weights[rows, columns])
                weights[rows, columns] = shrunk
                ahead[rows, columns] = advance
                low[rows, columns] = advance.astype(jnp.bfloat16)

        @pl.when(it < ITERS - 1)
        def _():
            predict(it + 1)

        wait_for(partial.at[it, 0], s(0))
        wait_for(half_in.at[it], s(2))
        wait_for(residual.at[it, 0], s(4))
        wait_for(arrived.at[it, pl.ds(0, TOK - 1)], s(6))
        wait_for(line_squares.at[it, pl.ds(0, 15)], s(8))
        wait_for(gathered.at[it, pl.ds(0, TOK - 1)], s(10))
        wait_for(plane_squares.at[it, pl.ds(0, 15)], s(12))
        return 0

    lax.fori_loop(0, ITERS, iteration, 0)


def shards(activations, dense_rows, targets):
    bf16, f32 = jnp.bfloat16, jnp.float32
    return pl.pallas_call(
        kernel,
        out_shape=pltpu.VMEM((ROWS, COLS), f32),
        in_specs=[pl.BlockSpec(memory_space=pltpu.HBM)] * 3,
        out_specs=pl.BlockSpec(memory_space=pltpu.VMEM),
        scratch_shapes=[
            pltpu.VMEM((TOKENS, COLS), bf16),
            pltpu.VMEM((ROWS, COLS), f32),
            pltpu.VMEM((ROWS, COLS), bf16),
            pltpu.VMEM((ROWS, TOKENS), f32),
            pltpu.VMEM((ITERS, 2, ROWS, HALF), f32),
            pltpu.VMEM((ITERS, ROWS, HALF), f32),
            pltpu.VMEM((ITERS, ROWS, HALF), bf16),
            pltpu.VMEM((ITERS, 3, ROWS, HALF), bf16),
            pltpu.VMEM((ITERS, 2, ROWS, HALF), bf16),
            pltpu.VMEM((ITERS, TOK, PIECE_ROWS, PIECE_COLS), bf16),
            pltpu.VMEM((ITERS, TOK, PIECE_ROWS, PIECE_COLS), bf16),
            pltpu.VMEM((ITERS, TOK, PIECE_ROWS, PIECE_COLS), bf16),
            pltpu.VMEM((ITERS, 16, 1, 128), f32),
            pltpu.VMEM((ITERS, 16, 1, 128), f32),
            pltpu.SemaphoreType.DMA((3,)),
            pltpu.SemaphoreType.DMA((ITERS, 14)),
        ],
        compiler_params=pltpu.CompilerParams(collective_id=0, has_side_effects=True),
    )(activations, dense_rows, targets.T)


def solution(mesh):
    in_specs = (P("tok", "feat"), P(None, "feat"), P("tok", None))
    out_specs = P(None, "feat")
    return jax.shard_map(shards, mesh=mesh, in_specs=in_specs, out_specs=out_specs, check_vma=False)
```

```python
import math

import jax
import jax.numpy as jnp
from jax import lax
from jax.experimental import pallas as pl
from jax.experimental.pallas import tpu as pltpu
from jax.sharding import PartitionSpec as P

DIN = 28672
ROWS = 64
ITERS = 4

step_size = 0.25
threshold = 0.2
epsilon = 1e-06

MESH = pl.DeviceIdType.MESH
FEAT = 8
TOK = 32
TOKENS = 256
HALF = ROWS // 2
COLS = DIN // FEAT
PIECE_ROWS = 8
PIECE_COLS = COLS // 4
TILES = PIECE_COLS // 128


def momentum_terms(iterations):
    values = []
    current = 1.0
    for _ in range(iterations):
        upcoming = (1.0 + math.sqrt(1.0 + 4.0 * current * current)) / 2.0
        values.append((current - 1.0) / upcoming)
        current = upcoming
    return values


def ring(offset, size):
    return min(offset, size - offset)


TOKEN_PEERS = sorted(
    [(dy, dz, dx) for dy in range(4) for dz in range(2) for dx in range(4) if (dy, dz, dx) != (0, 0, 0)],
    key=lambda o: -(ring(o[0], 4) + o[1] + ring(o[2], 4)),
)
LINE_PEERS = sorted(
    [(dz, dc) for dz in range(8) for dc in range(2) if (dz, dc) != (0, 0)], key=lambda o: -ring(o[0], 8) - o[1] / 2
)
PLANE_PEERS = sorted(
    [(dy, dx) for dy in range(4) for dx in range(4) if (dy, dx) != (0, 0)],
    key=lambda o: -(ring(o[0], 4) + ring(o[1], 4)),
)


COLUMN_PEERS = sorted([(dz, dx) for dz in range(2) for dx in range(4)], key=lambda o: -(o[0] + ring(o[1], 4)))


def kernel(
    act_hbm, dense_hbm, targets_hbm, weights,
    act, dense, goal, kept, ahead, pair_out, pair_in, product, half_out, half_in,
    pieces, arrived, gathered, line_squares, plane_squares,
    load_sem, pair_sem, sem,
):
    feat = lax.axis_index("feat")
    tok = lax.axis_index("tok")
    core = lax.rem(feat, 2)
    other = 1 - core
    partner = feat + 1 - 2 * core
    y, z_lo, x = tok // 8, lax.rem(tok // 4, 2), lax.rem(tok, 4)
    z = (feat // 2) * 2 + z_lo
    my_rows = pl.ds(pl.multiple_of(core * HALF, HALF), HALF)
    other_rows = pl.ds(pl.multiple_of(other * HALF, HALF), HALF)

    load_dense = pltpu.make_async_copy(dense_hbm, dense, load_sem.at[0])
    load_act = pltpu.make_async_copy(act_hbm, act.at[core], load_sem.at[1])
    load_goal = pltpu.make_async_copy(targets_hbm.at[my_rows], goal, load_sem.at[2])
    load_dense.start()
    load_act.start()
    load_goal.start()

    def token_peer(offset):
        dy, dz, dx = offset
        return lax.rem(y + dy, 4) * 8 + lax.rem(z_lo + dz, 2) * 4 + lax.rem(x + dx, 4)

    def line_peer(offset):
        dz, dc = offset
        to = lax.rem(z + dz, 8)
        return {"feat": (to // 2) * 2 + lax.rem(core + dc, 2), "tok": y * 8 + lax.rem(to, 2) * 4 + x}

    barrier = pltpu.get_barrier_semaphore()
    for offset in TOKEN_PEERS:
        pl.semaphore_signal(barrier, inc=1, device_id={"tok": token_peer(offset)}, device_id_type=MESH)
    for k in range(1, FEAT):
        pl.semaphore_signal(barrier, inc=1, device_id={"feat": lax.rem(feat + k, FEAT)}, device_id_type=MESH)

    def copy_to(src, dst, send, recv, device):
        pltpu.make_async_remote_copy(
            src_ref=src, dst_ref=dst, send_sem=send, recv_sem=recv, device_id=device, device_id_type=MESH
        ).start()

    def wait_for(ref, semaphore):
        pltpu.make_async_copy(ref, ref, semaphore).wait()

    contract_last = (((1,), (1,)), ((), ()))
    momentum = momentum_terms(ITERS)
    factor = DIN ** (-0.5)

    load_dense.wait()
    load_act.wait()
    first = lax.dot_general(
        dense[...].astype(jnp.bfloat16), act[core], contract_last, preferred_element_type=jnp.float32
    )
    pair_out[0] = first[:HALF]
    pair_out[1] = first[HALF:]
    kept[core] = dense[my_rows]
    ahead[core] = dense[my_rows]
    load_goal.wait()
    pl.semaphore_wait(barrier, TOK + FEAT - 2)
    copy_to(pair_out.at[other], pair_in, pair_sem.at[0], pair_sem.at[1], {"feat": partner})
    wait_for(pair_in, pair_sem.at[1])
    product[...] = pair_out[core] + pair_in[...]

    def iteration(it, _):
        def s(i):
            return sem.at[it, i]

        half = product[...]
        half_out[it] = half.astype(jnp.bfloat16)
        for k in (2, 1, 3):
            copy_to(half_out.at[it], half_in.at[it, k - 1], s(0), s(1), {"feat": lax.rem(feat + 2 * k, FEAT)})

        @pl.when(it == 0)
        def _():
            copy_to(act.at[core], act.at[core], pair_sem.at[2], pair_sem.at[3], {"feat": partner})
            copy_to(dense.at[other_rows], kept.at[core], pair_sem.at[4], pair_sem.at[5], {"feat": partner})

        wait_for(half_in.at[it], s(1))
        for k in range(3):
            half = half + half_in[it, k].astype(jnp.float32)
        residual = (factor * half - goal[...]).astype(jnp.bfloat16)

        @pl.when(it == 0)
        def _():
            wait_for(act.at[other], pair_sem.at[3])
            wait_for(kept.at[other], pair_sem.at[5])
            ahead[other] = kept[other]

        for dz, dx in COLUMN_PEERS:
            block, cx = lax.rem(z_lo + dz, 2), lax.rem(x + dx, 4)
            columns = pl.ds(pl.multiple_of(cx * PIECE_COLS, 128), PIECE_COLS)
            part = jnp.dot(residual, act[block, :, columns], preferred_element_type=jnp.float32)
            for g in range(4):
                pieces[it, g * 8 + block * 4 + cx] = part[g * 8 : g * 8 + 8].astype(jnp.bfloat16)
            for dy in (2, 1, 3, 0):
                if (dy, dz, dx) != (0, 0, 0):
                    to = token_peer((dy, dz, dx))
                    copy_to(pieces.at[it, to], arrived.at[it, tok], s(2), s(3), {"tok": to})
        arrived[it, tok] = pieces[it, tok]
        wait_for(arrived.at[it, pl.ds(0, TOK - 1)], s(3))
        total = arrived[it, 0].astype(jnp.float32)
        for p in range(1, TOK):
            total = total + arrived[it, p].astype(jnp.float32)
        gathered[it, tok] = total.astype(jnp.bfloat16)
        square = total * total
        lanes = square[:, :128]
        for c in range(1, TILES):
            lanes = lanes + square[:, c * 128 : c * 128 + 128]

        def spread(squares, slot, value, send, recv, devices):
            squares[it, slot] = value
            for device in devices:
                copy_to(squares.at[it, slot], squares.at[it, slot], send, recv, device)

        def collected(squares, recv):
            wait_for(squares.at[it, pl.ds(0, 15)], recv)
            sums = [squares[it, p] for p in range(16)]
            while len(sums) > 1:
                sums = [a + b for a, b in zip(sums[::2], sums[1::2])]
            return sums[0]

        spread(
            line_squares, z * 2 + core, jnp.sum(lanes, axis=0, keepdims=True), s(4), s(5),
            [line_peer(offset) for offset in LINE_PEERS],
        )
        for offset in TOKEN_PEERS:
            copy_to(gathered.at[it, tok], gathered.at[it, tok], s(6), s(7), {"tok": token_peer(offset)})
        spread(
            plane_squares, y * 4 + x, collected(line_squares, s(5)), s(8), s(9),
            [{"tok": token_peer((dy, 0, dx))} for dy, dx in PLANE_PEERS],
        )
        total_square = jnp.sum(collected(plane_squares, s(9)), axis=1, keepdims=True)
        scale = step_size * lax.rsqrt(total_square / (ROWS * DIN) + epsilon)
        m = jnp.float32(momentum[0])
        for i in range(1, ITERS):
            m = jnp.where(it == i, jnp.float32(momentum[i]), m)
        wait_for(gathered.at[it, pl.ds(0, TOK - 1)], s(7))

        def gradient_tile(block, r, t):
            tiles = [
                gathered[it, (2 * r + g) * 8 + block * 4 + t // TILES, :, (t % TILES) * 128 : (t % TILES) * 128 + 128]
                for g in range(2)
            ]
            return jnp.concatenate([tile.astype(jnp.float32) for tile in tiles], axis=0)

        def shrunk_tile(block, rows, columns, gradient):
            moved = ahead[block, rows, columns] - scale * gradient
            return moved - jnp.clip(moved, -threshold, threshold)

        @pl.when(it < ITERS - 1)
        def _():
            total = None
            for block in range(2):
                for chunk in range(7):
                    low = []
                    for r in range(2):
                        rows = slice(r * 16, r * 16 + 16)
                        line = []
                        for t in range(chunk * 4, chunk * 4 + 4):
                            columns = slice(t * 128, t * 128 + 128)
                            shrunk = shrunk_tile(block, rows, columns, gradient_tile(block, r, t))
                            advance = shrunk + m * (shrunk - kept[block, rows, columns])
                            kept[block, rows, columns] = shrunk
                            ahead[block, rows, columns] = advance
                            line.append(advance.astype(jnp.bfloat16))
                        low.append(jnp.concatenate(line, axis=1))
                    part = lax.dot_general(
                        jnp.concatenate(low, axis=0), act[block, :, chunk * 512 : chunk * 512 + 512],
                        contract_last, preferred_element_type=jnp.float32,
                    )
                    total = part if total is None else total + part
            product[...] = total

        @pl.when(it == ITERS - 1)
        def _():
            def finish(block, target, row_start, t):
                for r in range(2):
                    rows, columns = slice(r * 16, r * 16 + 16), slice(t * 128, t * 128 + 128)
                    shrunk = shrunk_tile(block, rows, columns, gradient_tile(block, r, t))
                    start = row_start + r * 16
                    if not isinstance(start, int):
                        start = pl.multiple_of(start, 16)
                    target[pl.ds(start, 16), columns] = shrunk

            for part in range(4):
                columns = pl.ds(part * PIECE_COLS, PIECE_COLS)
                for t in range(part * TILES, part * TILES + TILES):
                    finish(other, kept.at[other], 0, t)
                copy_to(
                    kept.at[other, :, columns], weights.at[my_rows, columns],
                    pair_sem.at[6], pair_sem.at[7], {"feat": partner},
                )
            for t in range(4 * TILES):
                finish(core, weights, core * HALF, t)
            wait_for(kept.at[core], pair_sem.at[7])
            wait_for(kept.at[core], pair_sem.at[6])

        wait_for(half_in.at[it], s(0))
        wait_for(arrived.at[it, pl.ds(0, TOK - 1)], s(2))
        wait_for(line_squares.at[it, pl.ds(0, 15)], s(4))
        wait_for(gathered.at[it, pl.ds(0, TOK - 1)], s(6))
        wait_for(plane_squares.at[it, pl.ds(0, 15)], s(8))
        return 0

    lax.fori_loop(0, ITERS, iteration, 0)
    wait_for(pair_in, pair_sem.at[0])
    wait_for(act.at[0], pair_sem.at[2])
    wait_for(kept.at[0], pair_sem.at[4])


def shards(activations, dense_rows, targets):
    bf16, f32 = jnp.bfloat16, jnp.float32
    piece_buffer = pltpu.VMEM((ITERS, TOK, PIECE_ROWS, PIECE_COLS), bf16)
    return pl.pallas_call(
        kernel,
        out_shape=pltpu.VMEM((ROWS, COLS), f32),
        in_specs=[pl.BlockSpec(memory_space=pltpu.HBM)] * 3,
        out_specs=pl.BlockSpec(memory_space=pltpu.VMEM),
        scratch_shapes=[
            pltpu.VMEM((2, TOKENS, COLS), bf16),
            pltpu.VMEM((ROWS, COLS), f32),
            pltpu.VMEM((HALF, TOKENS), f32),
            pltpu.VMEM((2, HALF, COLS), f32),
            pltpu.VMEM((2, HALF, COLS), f32),
            pltpu.VMEM((2, HALF, TOKENS), f32),
            pltpu.VMEM((HALF, TOKENS), f32),
            pltpu.VMEM((HALF, TOKENS), f32),
            pltpu.VMEM((ITERS, HALF, TOKENS), bf16),
            pltpu.VMEM((ITERS, 3, HALF, TOKENS), bf16),
            piece_buffer,
            piece_buffer,
            piece_buffer,
            pltpu.VMEM((ITERS, 16, 1, 128), f32),
            pltpu.VMEM((ITERS, 16, 1, 128), f32),
            pltpu.SemaphoreType.DMA((3,)),
            pltpu.SemaphoreType.DMA((8,)),
            pltpu.SemaphoreType.DMA((ITERS, 10)),
        ],
        compiler_params=pltpu.CompilerParams(collective_id=0, has_side_effects=True),
    )(activations, dense_rows, targets.T)


def solution(mesh):
    in_specs = (P("tok", "feat"), P(None, "feat"), P("tok", None))
    out_specs = P(None, "feat")
    return jax.shard_map(shards, mesh=mesh, in_specs=in_specs, out_specs=out_specs, check_vma=False)
```

```python
import math

import jax
import jax.numpy as jnp
from jax import lax
from jax.experimental import pallas as pl
from jax.experimental.pallas import tpu as pltpu
from jax.sharding import PartitionSpec as P

DIN = 28672
ROWS = 64
ITERS = 4

step_size = 0.25
threshold = 0.2
epsilon = 1e-06

MESH = pl.DeviceIdType.MESH
FEAT = 8
TOK = 32
TOKENS = 256
COLS = DIN // FEAT
PIECE_ROWS = 16
PIECE_COLS = COLS // 4
TILES = PIECE_COLS // 128


def momentum_terms(iterations):
    values = []
    current = 1.0
    for _ in range(iterations):
        upcoming = (1.0 + math.sqrt(1.0 + 4.0 * current * current)) / 2.0
        values.append((current - 1.0) / upcoming)
        current = upcoming
    return values


def ring(offset, size):
    return min(offset, size - offset)


TOKEN_PEERS = sorted(
    [(dy, dz, dx) for dy in range(4) for dz in range(2) for dx in range(4) if (dy, dz, dx) != (0, 0, 0)],
    key=lambda o: -(ring(o[0], 4) + o[1] + ring(o[2], 4)),
)
LINE_PEERS = sorted(range(1, 8), key=lambda o: -ring(o, 8))
PLANE_PEERS = sorted(
    [(dy, dx) for dy in range(4) for dx in range(4) if (dy, dx) != (0, 0)],
    key=lambda o: -(ring(o[0], 4) + ring(o[1], 4)),
)


COLUMN_PEERS = sorted([(dz, dx) for dz in range(2) for dx in range(4)], key=lambda o: -(o[0] + ring(o[1], 4)))


def kernel(
    act_hbm, dense_hbm, targets_hbm, weights,
    act, goal, kept, ahead, pair_out, pair_in, product, part_out, part_in,
    pieces, arrived, gathered, line_squares, plane_squares,
    load_sem, pair_sem, sem,
):
    feat = lax.axis_index("feat")
    tok = lax.axis_index("tok")
    core = lax.rem(feat, 2)
    partner = {"feat": feat + 1 - 2 * core}

    load_dense = pltpu.make_async_copy(dense_hbm, kept.at[core], load_sem.at[0])
    load_act = pltpu.make_async_copy(act_hbm, act.at[core], load_sem.at[1])
    load_goal = pltpu.make_async_copy(targets_hbm, goal, load_sem.at[2])
    load_dense.start()
    load_act.start()
    load_goal.start()

    barrier = pltpu.get_barrier_semaphore()
    pl.semaphore_signal(barrier, inc=1, device_id=partner, device_id_type=MESH)

    def copy_to(src, dst, send, recv, device):
        pltpu.make_async_remote_copy(
            src_ref=src, dst_ref=dst, send_sem=send, recv_sem=recv, device_id=device, device_id_type=MESH
        ).start()

    def wait_for(ref, semaphore):
        pltpu.make_async_copy(ref, ref, semaphore).wait()

    contract_last = (((1,), (1,)), ((), ()))

    def first_product():
        load_dense.wait()
        load_act.wait()
        load_goal.wait()
        return lax.dot_general(
            kept[core].astype(jnp.bfloat16), act[core], contract_last, preferred_element_type=jnp.float32
        )

    @pl.when(core == 0)
    def _():
        pair_out[...] = first_product()
        pl.semaphore_wait(barrier, 1)
        copy_to(pair_out, pair_in, pair_sem.at[0], pair_sem.at[1], partner)
        copy_to(act.at[0], act.at[0], pair_sem.at[2], pair_sem.at[3], partner)
        copy_to(kept.at[0], kept.at[0], pair_sem.at[4], pair_sem.at[5], partner)
        wait_for(pair_out, pair_sem.at[0])
        wait_for(act.at[0], pair_sem.at[2])
        wait_for(kept.at[0], pair_sem.at[4])
        wait_for(kept.at[0], pair_sem.at[7])

    @pl.when(core == 1)
    def _():
        y, z_lo, x = tok // 8, lax.rem(tok // 4, 2), lax.rem(tok, 4)
        z = (feat // 2) * 2 + z_lo

        def token_peer(offset):
            dy, dz, dx = offset
            return lax.rem(y + dy, 4) * 8 + lax.rem(z_lo + dz, 2) * 4 + lax.rem(x + dx, 4)

        def line_peer(dz):
            to = lax.rem(z + dz, 8)
            return {"feat": (to // 2) * 2 + 1, "tok": y * 8 + lax.rem(to, 2) * 4 + x}

        for offset in TOKEN_PEERS:
            pl.semaphore_signal(barrier, inc=1, device_id={"tok": token_peer(offset)}, device_id_type=MESH)
        for k in (2, 1, 3):
            pl.semaphore_signal(
                barrier, inc=1, device_id={"feat": lax.rem(feat + 2 * k, FEAT)}, device_id_type=MESH
            )
        momentum = momentum_terms(ITERS)
        factor = DIN ** (-0.5)
        product[...] = first_product()
        ahead[1] = kept[1]
        pl.semaphore_wait(barrier, TOK + FEAT // 2 - 1)
        wait_for(pair_in, pair_sem.at[1])
        product[...] += pair_in[...]

        def iteration(it, _):
            def s(i):
                return sem.at[it, i]

            own = product[...]
            part_out[it] = own.astype(jnp.bfloat16)
            for k in (2, 1, 3):
                copy_to(part_out.at[it], part_in.at[it, k - 1], s(0), s(1), {"feat": lax.rem(feat + 2 * k, FEAT)})
            wait_for(part_in.at[it], s(1))
            for k in range(3):
                own = own + part_in[it, k].astype(jnp.float32)
            residual = (factor * own - goal[...]).astype(jnp.bfloat16)

            @pl.when(it == 0)
            def _():
                wait_for(act.at[0], pair_sem.at[3])

            for dz, dx in COLUMN_PEERS:
                block, cx = lax.rem(z_lo + dz, 2), lax.rem(x + dx, 4)
                columns = pl.ds(pl.multiple_of(cx * PIECE_COLS, 128), PIECE_COLS)
                part = jnp.dot(residual, act[block, :, columns], preferred_element_type=jnp.float32)
                for g in range(4):
                    pieces[it, g * 8 + block * 4 + cx] = part[g * 16 : g * 16 + 16].astype(jnp.bfloat16)
                for dy in (2, 1, 3, 0):
                    if (dy, dz, dx) != (0, 0, 0):
                        to = token_peer((dy, dz, dx))
                        copy_to(pieces.at[it, to], arrived.at[it, tok], s(2), s(3), {"tok": to})
            arrived[it, tok] = pieces[it, tok]

            @pl.when(it == 0)
            def _():
                wait_for(kept.at[0], pair_sem.at[5])
                ahead[0] = kept[0]

            wait_for(arrived.at[it, pl.ds(0, TOK - 1)], s(3))
            total = arrived[it, 0].astype(jnp.float32)
            for p in range(1, TOK):
                total = total + arrived[it, p].astype(jnp.float32)
            gathered[it, tok] = total.astype(jnp.bfloat16)
            square = total * total
            square = square[:8] + square[8:]
            lanes = square[:, :128]
            for c in range(1, TILES):
                lanes = lanes + square[:, c * 128 : c * 128 + 128]

            def spread(squares, slot, value, send, recv, devices):
                squares[it, slot] = value
                for device in devices:
                    copy_to(squares.at[it, slot], squares.at[it, slot], send, recv, device)

            def collected(squares, recv, number):
                wait_for(squares.at[it, pl.ds(0, number - 1)], recv)
                sums = [squares[it, p] for p in range(number)]
                while len(sums) > 1:
                    sums = [a + b for a, b in zip(sums[::2], sums[1::2])]
                return sums[0]

            spread(
                line_squares, z, jnp.sum(lanes, axis=0, keepdims=True), s(4), s(5),
                [line_peer(dz) for dz in LINE_PEERS],
            )
            for offset in TOKEN_PEERS:
                copy_to(gathered.at[it, tok], gathered.at[it, tok], s(6), s(7), {"tok": token_peer(offset)})
            spread(
                plane_squares, y * 4 + x, collected(line_squares, s(5), 8), s(8), s(9),
                [{"tok": token_peer((dy, 0, dx))} for dy, dx in PLANE_PEERS],
            )
            total_square = jnp.sum(collected(plane_squares, s(9), 16), axis=1, keepdims=True)
            scale = step_size * lax.rsqrt(total_square / (ROWS * DIN) + epsilon)
            m = jnp.float32(momentum[0])
            for i in range(1, ITERS):
                m = jnp.where(it == i, jnp.float32(momentum[i]), m)
            wait_for(gathered.at[it, pl.ds(0, TOK - 1)], s(7))

            def shrunk_tile(block, r, t):
                rows, columns = slice(r * 16, r * 16 + 16), slice(t * 128, t * 128 + 128)
                inner = slice((t % TILES) * 128, (t % TILES) * 128 + 128)
                gradient = gathered[it, r * 8 + block * 4 + t // TILES, :, inner].astype(jnp.float32)
                moved = ahead[block, rows, columns] - scale * gradient
                return rows, columns, moved - jnp.clip(moved, -threshold, threshold)

            @pl.when(it < ITERS - 1)
            def _():
                total = None
                for block in range(2):
                    for chunk in range(7):
                        low = []
                        for r in range(4):
                            line = []
                            for t in range(chunk * 4, chunk * 4 + 4):
                                rows, columns, shrunk = shrunk_tile(block, r, t)
                                advance = shrunk + m * (shrunk - kept[block, rows, columns])
                                kept[block, rows, columns] = shrunk
                                ahead[block, rows, columns] = advance
                                line.append(advance.astype(jnp.bfloat16))
                            low.append(jnp.concatenate(line, axis=1))
                        part = lax.dot_general(
                            jnp.concatenate(low, axis=0), act[block, :, chunk * 512 : chunk * 512 + 512],
                            contract_last, preferred_element_type=jnp.float32,
                        )
                        total = part if total is None else total + part
                product[...] = total

            @pl.when(it == ITERS - 1)
            def _():
                for part in range(4):
                    block_columns = pl.ds(part * PIECE_COLS, PIECE_COLS)
                    for t in range(part * TILES, part * TILES + TILES):
                        for r in range(4):
                            rows, columns, shrunk = shrunk_tile(0, r, t)
                            kept[0, rows, columns] = shrunk
                    copy_to(
                        kept.at[0, :, block_columns], weights.at[:, block_columns],
                        pair_sem.at[6], pair_sem.at[7], partner,
                    )
                for t in range(4 * TILES):
                    for r in range(4):
                        rows, columns, shrunk = shrunk_tile(1, r, t)
                        weights[rows, columns] = shrunk
                wait_for(kept.at[0], pair_sem.at[6])

            wait_for(part_in.at[it], s(0))
            wait_for(arrived.at[it, pl.ds(0, TOK - 1)], s(2))
            wait_for(line_squares.at[it, pl.ds(0, 7)], s(4))
            wait_for(gathered.at[it, pl.ds(0, TOK - 1)], s(6))
            wait_for(plane_squares.at[it, pl.ds(0, 15)], s(8))
            return 0

        lax.fori_loop(0, ITERS, iteration, 0)


def shards(activations, dense_rows, targets):
    bf16, f32 = jnp.bfloat16, jnp.float32
    piece_buffer = pltpu.VMEM((ITERS, TOK, PIECE_ROWS, PIECE_COLS), bf16)
    return pl.pallas_call(
        kernel,
        out_shape=pltpu.VMEM((ROWS, COLS), f32),
        in_specs=[pl.BlockSpec(memory_space=pltpu.HBM)] * 3,
        out_specs=pl.BlockSpec(memory_space=pltpu.VMEM),
        scratch_shapes=[
            pltpu.VMEM((2, TOKENS, COLS), bf16),
            pltpu.VMEM((ROWS, TOKENS), f32),
            pltpu.VMEM((2, ROWS, COLS), f32),
            pltpu.VMEM((2, ROWS, COLS), f32),
            pltpu.VMEM((ROWS, TOKENS), f32),
            pltpu.VMEM((ROWS, TOKENS), f32),
            pltpu.VMEM((ROWS, TOKENS), f32),
            pltpu.VMEM((ITERS, ROWS, TOKENS), bf16),
            pltpu.VMEM((ITERS, 3, ROWS, TOKENS), bf16),
            piece_buffer,
            piece_buffer,
            piece_buffer,
            pltpu.VMEM((ITERS, 8, 1, 128), f32),
            pltpu.VMEM((ITERS, 16, 1, 128), f32),
            pltpu.SemaphoreType.DMA((3,)),
            pltpu.SemaphoreType.DMA((8,)),
            pltpu.SemaphoreType.DMA((ITERS, 10)),
        ],
        compiler_params=pltpu.CompilerParams(collective_id=0, has_side_effects=True),
    )(activations, dense_rows, targets.T)


def solution(mesh):
    in_specs = (P("tok", "feat"), P(None, "feat"), P("tok", None))
    out_specs = P(None, "feat")
    return jax.shard_map(shards, mesh=mesh, in_specs=in_specs, out_specs=out_specs, check_vma=False)
```

```python
import math

import jax
import jax.numpy as jnp
from jax import lax
from jax.experimental import pallas as pl
from jax.experimental.pallas import tpu as pltpu
from jax.sharding import PartitionSpec as P

DIN = 28672
ROWS = 64
ITERS = 4

step_size = 0.25
threshold = 0.2
epsilon = 1e-06

RS_N, RS_S = (2, 1), (3, 0)
AG_N, AG_S = (2,), (1, 3, 0)
MESH = pl.DeviceIdType.MESH
FEAT = 8
TOK = 32
TOKENS = 256
COLS = DIN // FEAT
PIECE_ROWS = 16
PIECE_COLS = COLS // 4
TILES = PIECE_COLS // 128


def momentum_terms(iterations):
    values = []
    current = 1.0
    for _ in range(iterations):
        upcoming = (1.0 + math.sqrt(1.0 + 4.0 * current * current)) / 2.0
        values.append((current - 1.0) / upcoming)
        current = upcoming
    return values


def ring(offset, size):
    return min(offset, size - offset)


TOKEN_PEERS = sorted(
    [(dy, dz, dx) for dy in range(4) for dz in range(2) for dx in range(4) if (dy, dz, dx) != (0, 0, 0)],
    key=lambda o: -(ring(o[0], 4) + o[1] + ring(o[2], 4)),
)
LINE_PEERS = sorted(range(1, 8), key=lambda o: -ring(o, 8))
PLANE_PEERS = sorted(
    [(dy, dx) for dy in range(4) for dx in range(4) if (dy, dx) != (0, 0)],
    key=lambda o: -(ring(o[0], 4) + ring(o[1], 4)),
)


COLUMN_PEERS = sorted([(dz, dx) for dz in range(2) for dx in range(4)], key=lambda o: -(o[0] + ring(o[1], 4)))


def kernel(
    act_hbm, dense_hbm, targets_hbm, weights,
    act, goal, kept, ahead, pair_out, pair_in, product, part_out, part_in, residual,
    pieces, arrived, gathered, line_squares, plane_squares,
    load_sem, pair_sem, sem,
):
    feat = lax.axis_index("feat")
    tok = lax.axis_index("tok")
    core = lax.rem(feat, 2)
    y, z_lo, x = tok // 8, lax.rem(tok // 4, 2), lax.rem(tok, 4)
    z = (feat // 2) * 2 + z_lo
    partner = {"feat": feat + 1 - 2 * core}

    load_dense = pltpu.make_async_copy(dense_hbm, kept.at[core], load_sem.at[0])
    load_act = pltpu.make_async_copy(act_hbm, act.at[core], load_sem.at[1])
    load_goal = pltpu.make_async_copy(targets_hbm, goal, load_sem.at[2])
    load_dense.start()
    load_act.start()
    load_goal.start()

    barrier = pltpu.get_barrier_semaphore()
    pl.semaphore_signal(barrier, inc=1, device_id=partner, device_id_type=MESH)

    def copy_to(src, dst, send, recv, device):
        pltpu.make_async_remote_copy(
            src_ref=src, dst_ref=dst, send_sem=send, recv_sem=recv, device_id=device, device_id_type=MESH
        ).start()

    def wait_for(ref, semaphore):
        pltpu.make_async_copy(ref, ref, semaphore).wait()

    contract_last = (((1,), (1,)), ((), ()))

    def first_product():
        load_dense.wait()
        load_act.wait()
        load_goal.wait()
        return lax.dot_general(
            kept[core].astype(jnp.bfloat16), act[core], contract_last, preferred_element_type=jnp.float32
        )

    def token_peer(offset):
        dy, dz, dx = offset
        return lax.rem(y + dy, 4) * 8 + lax.rem(z_lo + dz, 2) * 4 + lax.rem(x + dx, 4)

    def send_pieces(it, offsets):
        residuals = jnp.concatenate([residual[it, lax.rem(y + dy, 4)] for dy in offsets], axis=0)
        for dz, dx in COLUMN_PEERS:
            block, cx = lax.rem(z_lo + dz, 2), lax.rem(x + dx, 4)
            columns = pl.ds(pl.multiple_of(cx * PIECE_COLS, 128), PIECE_COLS)
            part = jnp.dot(residuals, act[block, :, columns], preferred_element_type=jnp.float32)
            for i, dy in enumerate(offsets):
                to = token_peer((dy, dz, dx))
                pieces[it, to] = part[i * 16 : i * 16 + 16].astype(jnp.bfloat16)
                copy_to(
                    pieces.at[it, to], arrived.at[it, tok], sem.at[it, 2], sem.at[it, 3],
                    {"feat": feat + 1 - core, "tok": to} if (dy, dz, dx) != (0, 0, 0) else partner,
                )

    def send_gradient(it, offsets):
        for offset in TOKEN_PEERS:
            if offset[0] in offsets:
                copy_to(
                    gathered.at[it, tok], gathered.at[it, tok], sem.at[it, 6], sem.at[it, 7],
                    {"feat": feat + 1 - core, "tok": token_peer(offset)},
                )

    @pl.when(core == 0)
    def _():
        pair_out[...] = first_product()
        pl.semaphore_wait(barrier, 1)
        copy_to(pair_out, pair_in, pair_sem.at[0], pair_sem.at[1], partner)
        copy_to(act.at[0], act.at[0], pair_sem.at[2], pair_sem.at[3], partner)
        copy_to(kept.at[0], kept.at[0], pair_sem.at[4], pair_sem.at[5], partner)
        wait_for(pair_out, pair_sem.at[0])
        wait_for(act.at[0], pair_sem.at[2])
        wait_for(act.at[1], pair_sem.at[3])

        def help_out(it, _):
            wait_for(residual.at[it], sem.at[it, 11])
            send_pieces(it, RS_S)
            wait_for(gathered.at[it, tok], sem.at[it, 13])
            send_gradient(it, AG_S)
            wait_for(pieces.at[it, pl.ds(0, 8 * len(RS_S))], sem.at[it, 2])
            wait_for(gathered.at[it, pl.ds(0, 8 * len(AG_S) - (0 in AG_S))], sem.at[it, 6])
            return 0

        lax.fori_loop(0, ITERS, help_out, 0)
        wait_for(kept.at[0], pair_sem.at[4])
        wait_for(kept.at[0], pair_sem.at[7])

    @pl.when(core == 1)
    def _():
        def line_peer(dz):
            to = lax.rem(z + dz, 8)
            return {"feat": (to // 2) * 2 + 1, "tok": y * 8 + lax.rem(to, 2) * 4 + x}

        for offset in TOKEN_PEERS:
            pl.semaphore_signal(barrier, inc=1, device_id={"tok": token_peer(offset)}, device_id_type=MESH)
        for k in (2, 1, 3):
            pl.semaphore_signal(
                barrier, inc=1, device_id={"feat": lax.rem(feat + 2 * k, FEAT)}, device_id_type=MESH
            )
        momentum = momentum_terms(ITERS)
        factor = DIN ** (-0.5)
        product[...] = first_product()
        ahead[1] = kept[1]
        pl.semaphore_wait(barrier, TOK + FEAT // 2 - 1)
        copy_to(act.at[1], act.at[1], pair_sem.at[2], pair_sem.at[3], partner)
        wait_for(pair_in, pair_sem.at[1])
        product[...] += pair_in[...]

        def iteration(it, _):
            def s(i):
                return sem.at[it, i]

            own = product[...]
            part_out[it] = own.astype(jnp.bfloat16)
            for k in (2, 1, 3):
                copy_to(part_out.at[it], part_in.at[it, k - 1], s(0), s(1), {"feat": lax.rem(feat + 2 * k, FEAT)})
            wait_for(part_in.at[it], s(1))
            for k in range(3):
                own = own + part_in[it, k].astype(jnp.float32)
            left = (factor * own - goal[...]).astype(jnp.bfloat16)
            for g in range(4):
                residual[it, g] = left[g * 16 : g * 16 + 16]
            copy_to(residual.at[it], residual.at[it], s(10), s(11), partner)

            @pl.when(it == 0)
            def _():
                wait_for(act.at[0], pair_sem.at[3])

            send_pieces(it, RS_N)

            @pl.when(it == 0)
            def _():
                wait_for(kept.at[0], pair_sem.at[5])
                ahead[0] = kept[0]

            wait_for(arrived.at[it], s(3))
            total = arrived[it, 0].astype(jnp.float32)
            for p in range(1, TOK):
                total = total + arrived[it, p].astype(jnp.float32)
            gathered[it, tok] = total.astype(jnp.bfloat16)
            square = total * total
            square = square[:8] + square[8:]
            lanes = square[:, :128]
            for c in range(1, TILES):
                lanes = lanes + square[:, c * 128 : c * 128 + 128]

            def spread(squares, slot, value, send, recv, devices):
                squares[it, slot] = value
                for device in devices:
                    copy_to(squares.at[it, slot], squares.at[it, slot], send, recv, device)

            def collected(squares, recv, number):
                wait_for(squares.at[it, pl.ds(0, number - 1)], recv)
                sums = [squares[it, p] for p in range(number)]
                while len(sums) > 1:
                    sums = [a + b for a, b in zip(sums[::2], sums[1::2])]
                return sums[0]

            spread(
                line_squares, z, jnp.sum(lanes, axis=0, keepdims=True), s(4), s(5),
                [line_peer(dz) for dz in LINE_PEERS],
            )
            copy_to(gathered.at[it, tok], gathered.at[it, tok], s(12), s(13), partner)
            send_gradient(it, AG_N)
            spread(
                plane_squares, y * 4 + x, collected(line_squares, s(5), 8), s(8), s(9),
                [{"tok": token_peer((dy, 0, dx))} for dy, dx in PLANE_PEERS],
            )
            total_square = jnp.sum(collected(plane_squares, s(9), 16), axis=1, keepdims=True)
            scale = step_size * lax.rsqrt(total_square / (ROWS * DIN) + epsilon)
            m = jnp.float32(momentum[0])
            for i in range(1, ITERS):
                m = jnp.where(it == i, jnp.float32(momentum[i]), m)
            wait_for(gathered.at[it, pl.ds(0, TOK - 1)], s(7))

            def shrunk_tile(block, r, t):
                rows, columns = slice(r * 16, r * 16 + 16), slice(t * 128, t * 128 + 128)
                inner = slice((t % TILES) * 128, (t % TILES) * 128 + 128)
                gradient = gathered[it, r * 8 + block * 4 + t // TILES, :, inner].astype(jnp.float32)
                moved = ahead[block, rows, columns] - scale * gradient
                return rows, columns, moved - jnp.clip(moved, -threshold, threshold)

            @pl.when(it < ITERS - 1)
            def _():
                total = None
                for block in range(2):
                    for chunk in range(7):
                        low = []
                        for r in range(4):
                            line = []
                            for t in range(chunk * 4, chunk * 4 + 4):
                                rows, columns, shrunk = shrunk_tile(block, r, t)
                                advance = shrunk + m * (shrunk - kept[block, rows, columns])
                                kept[block, rows, columns] = shrunk
                                ahead[block, rows, columns] = advance
                                line.append(advance.astype(jnp.bfloat16))
                            low.append(jnp.concatenate(line, axis=1))
                        part = lax.dot_general(
                            jnp.concatenate(low, axis=0), act[block, :, chunk * 512 : chunk * 512 + 512],
                            contract_last, preferred_element_type=jnp.float32,
                        )
                        total = part if total is None else total + part
                product[...] = total

            @pl.when(it == ITERS - 1)
            def _():
                for part in range(4):
                    block_columns = pl.ds(part * PIECE_COLS, PIECE_COLS)
                    for t in range(part * TILES, part * TILES + TILES):
                        for r in range(4):
                            rows, columns, shrunk = shrunk_tile(0, r, t)
                            kept[0, rows, columns] = shrunk
                    copy_to(
                        kept.at[0, :, block_columns], weights.at[:, block_columns],
                        pair_sem.at[6], pair_sem.at[7], partner,
                    )
                for t in range(4 * TILES):
                    for r in range(4):
                        rows, columns, shrunk = shrunk_tile(1, r, t)
                        weights[rows, columns] = shrunk
                wait_for(kept.at[0], pair_sem.at[6])

            wait_for(part_in.at[it], s(0))
            wait_for(pieces.at[it, pl.ds(0, 8 * len(RS_N))], s(2))
            wait_for(line_squares.at[it, pl.ds(0, 7)], s(4))
            wait_for(gathered.at[it, pl.ds(0, 8 * len(AG_N) - (0 in AG_N))], s(6))
            wait_for(residual.at[it], s(10))
            wait_for(gathered.at[it, tok], s(12))
            wait_for(plane_squares.at[it, pl.ds(0, 15)], s(8))
            return 0

        lax.fori_loop(0, ITERS, iteration, 0)
        wait_for(act.at[1], pair_sem.at[2])


def shards(activations, dense_rows, targets):
    bf16, f32 = jnp.bfloat16, jnp.float32
    piece_buffer = pltpu.VMEM((ITERS, TOK, PIECE_ROWS, PIECE_COLS), bf16)
    return pl.pallas_call(
        kernel,
        out_shape=pltpu.VMEM((ROWS, COLS), f32),
        in_specs=[pl.BlockSpec(memory_space=pltpu.HBM)] * 3,
        out_specs=pl.BlockSpec(memory_space=pltpu.VMEM),
        scratch_shapes=[
            pltpu.VMEM((2, TOKENS, COLS), bf16),
            pltpu.VMEM((ROWS, TOKENS), f32),
            pltpu.VMEM((2, ROWS, COLS), f32),
            pltpu.VMEM((2, ROWS, COLS), f32),
            pltpu.VMEM((ROWS, TOKENS), f32),
            pltpu.VMEM((ROWS, TOKENS), f32),
            pltpu.VMEM((ROWS, TOKENS), f32),
            pltpu.VMEM((ITERS, ROWS, TOKENS), bf16),
            pltpu.VMEM((ITERS, 3, ROWS, TOKENS), bf16),
            pltpu.VMEM((ITERS, 4, 16, TOKENS), bf16),
            piece_buffer,
            piece_buffer,
            piece_buffer,
            pltpu.VMEM((ITERS, 8, 1, 128), f32),
            pltpu.VMEM((ITERS, 16, 1, 128), f32),
            pltpu.SemaphoreType.DMA((3,)),
            pltpu.SemaphoreType.DMA((8,)),
            pltpu.SemaphoreType.DMA((ITERS, 14)),
        ],
        compiler_params=pltpu.CompilerParams(collective_id=0, has_side_effects=True),
    )(activations, dense_rows, targets.T)


def solution(mesh):
    in_specs = (P("tok", "feat"), P(None, "feat"), P("tok", None))
    out_specs = P(None, "feat")
    return jax.shard_map(shards, mesh=mesh, in_specs=in_specs, out_specs=out_specs, check_vma=False)
```

```python
import math

import jax
import jax.numpy as jnp
from jax import lax
from jax.experimental import pallas as pl
from jax.experimental.pallas import tpu as pltpu
from jax.sharding import PartitionSpec as P

DIN = 28672
ROWS = 64
ITERS = 4

step_size = 0.25
threshold = 0.2
epsilon = 1e-06

AG_N, AG_S = (2,), (1, 3, 0)
MESH = pl.DeviceIdType.MESH
FEAT = 8
TOK = 32
TOKENS = 256
COLS = DIN // FEAT
PIECE_ROWS = 16
PIECE_COLS = COLS // 4
TILES = PIECE_COLS // 128


def momentum_terms(iterations):
    values = []
    current = 1.0
    for _ in range(iterations):
        upcoming = (1.0 + math.sqrt(1.0 + 4.0 * current * current)) / 2.0
        values.append((current - 1.0) / upcoming)
        current = upcoming
    return values


def ring(offset, size):
    return min(offset, size - offset)


TOKEN_PEERS = sorted(
    [(dy, dz, dx) for dy in range(4) for dz in range(2) for dx in range(4) if (dy, dz, dx) != (0, 0, 0)],
    key=lambda o: -(ring(o[0], 4) + o[1] + ring(o[2], 4)),
)
LINE_PEERS = sorted(range(1, 8), key=lambda o: -ring(o, 8))
PLANE_PEERS = sorted(
    [(dy, dx) for dy in range(4) for dx in range(4) if (dy, dx) != (0, 0)],
    key=lambda o: -(ring(o[0], 4) + ring(o[1], 4)),
)


COLUMN_PEERS = sorted([(dz, dx) for dz in range(2) for dx in range(4)], key=lambda o: -(o[0] + ring(o[1], 4)))


def kernel(
    act_hbm, dense_hbm, targets_hbm, weights,
    act, goal, kept, ahead, pair_out, pair_in, product, part_out, part_in, residual,
    pieces, arrived, gathered, line_squares, plane_squares, plane_sum,
    load_sem, pair_sem, sem,
):
    feat = lax.axis_index("feat")
    tok = lax.axis_index("tok")
    core = lax.rem(feat, 2)
    y, z_lo, x = tok // 8, lax.rem(tok // 4, 2), lax.rem(tok, 4)
    z = (feat // 2) * 2 + z_lo
    partner = {"feat": feat + 1 - 2 * core}

    def token_peer(offset):
        dy, dz, dx = offset
        return lax.rem(y + dy, 4) * 8 + lax.rem(z_lo + dz, 2) * 4 + lax.rem(x + dx, 4)

    barrier = pltpu.get_barrier_semaphore()

    @pl.when(core == 1)
    def _():
        for offset in TOKEN_PEERS:
            pl.semaphore_signal(barrier, inc=1, device_id={"tok": token_peer(offset)}, device_id_type=MESH)
        for k in (2, 1, 3):
            pl.semaphore_signal(
                barrier, inc=1, device_id={"feat": lax.rem(feat + 2 * k, FEAT)}, device_id_type=MESH
            )

    pl.semaphore_signal(barrier, inc=1, device_id=partner, device_id_type=MESH)
    load_dense = pltpu.make_async_copy(dense_hbm, kept.at[core], load_sem.at[0])
    load_act = pltpu.make_async_copy(act_hbm, act.at[core], load_sem.at[1])
    load_goal = pltpu.make_async_copy(targets_hbm, goal, load_sem.at[2])
    load_dense.start()
    load_act.start()
    load_goal.start()

    def copy_to(src, dst, send, recv, device):
        pltpu.make_async_remote_copy(
            src_ref=src, dst_ref=dst, send_sem=send, recv_sem=recv, device_id=device, device_id_type=MESH
        ).start()

    def wait_for(ref, semaphore):
        pltpu.make_async_copy(ref, ref, semaphore).wait()

    contract_last = (((1,), (1,)), ((), ()))

    def first_product():
        load_dense.wait()
        load_act.wait()
        load_goal.wait()
        return lax.dot_general(
            kept[core].astype(jnp.bfloat16), act[core], contract_last, preferred_element_type=jnp.float32
        )

    def send_pieces(it):
        residuals = residual[it, core]
        arrival = sem.at[it, 14 - 11 * core]
        for dz, dx in COLUMN_PEERS:
            block, cx = lax.rem(z_lo + dz, 2), lax.rem(x + dx, 4)
            columns = pl.ds(pl.multiple_of(cx * PIECE_COLS, 128), PIECE_COLS)
            part = jnp.dot(residuals, act[block, :, columns], preferred_element_type=jnp.float32)
            for g in range(4):
                pieces[it, core, g * 8 + block * 4 + cx] = part[g * 8 : g * 8 + 8].astype(jnp.bfloat16)
            for dy in (2, 1, 3, 0):
                if (dy, dz, dx) != (0, 0, 0):
                    to = token_peer((dy, dz, dx))
                    copy_to(
                        pieces.at[it, core, to], arrived.at[it, core, tok], sem.at[it, 2], arrival,
                        {"feat": feat + 1 - core, "tok": to},
                    )

    def send_gradient(it, offsets):
        target = feat - core + jnp.where(it == ITERS - 1, z_lo, 1)
        for offset in TOKEN_PEERS:
            if offset[0] in offsets:
                copy_to(
                    gathered.at[it, tok], gathered.at[it, tok], sem.at[it, 6], sem.at[it, 7],
                    {"feat": target, "tok": token_peer(offset)},
                )

    def wait_for_last_gradient(it):
        @pl.when(z_lo == core)
        def _():
            wait_for(gathered.at[it, pl.ds(0, TOK // 2 - 1)], sem.at[it, 7])

        @pl.when(z_lo != core)
        def _():
            wait_for(gathered.at[it, pl.ds(0, TOK // 2)], sem.at[it, 7])

    def step_scale(lanes):
        total_square = jnp.sum(lanes, axis=1, keepdims=True)
        return step_size * lax.rsqrt(total_square / (ROWS * DIN) + epsilon)

    def shrunk_tile(it, scale, block, r, t):
        rows, columns = slice(r * 16, r * 16 + 16), slice(t * 128, t * 128 + 128)
        inner = slice((t % TILES) * 128, (t % TILES) * 128 + 128)
        gradient = gathered[it, r * 8 + block * 4 + t // TILES, :, inner].astype(jnp.float32)
        moved = ahead[block, rows, columns] - scale * gradient
        return rows, columns, moved - jnp.clip(moved, -threshold, threshold)

    def finish(it, scale, block):
        for t in range(4 * TILES):
            for r in range(4):
                rows, columns, shrunk = shrunk_tile(it, scale, block, r, t)
                weights[rows, columns] = shrunk

    @pl.when(core == 0)
    def _():
        pair_out[...] = first_product()
        pl.semaphore_wait(barrier, 1)
        copy_to(pair_out, pair_in, pair_sem.at[0], pair_sem.at[1], partner)
        copy_to(act.at[0], act.at[0], pair_sem.at[2], pair_sem.at[3], partner)
        copy_to(kept.at[0], kept.at[0], pair_sem.at[4], pair_sem.at[5], partner)
        wait_for(pair_out, pair_sem.at[0])
        wait_for(act.at[0], pair_sem.at[2])
        wait_for(act.at[1], pair_sem.at[3])

        def help_out(it, _):
            wait_for(residual.at[it, 0], sem.at[it, 11])
            send_pieces(it)
            copy_to(pieces.at[it, 0, tok], arrived.at[it, 0, tok], sem.at[it, 2], sem.at[it, 14], partner)
            wait_for(gathered.at[it, tok], sem.at[it, 13])
            send_gradient(it, AG_S)
            wait_for(pieces.at[it, 0], sem.at[it, 2])
            wait_for(gathered.at[it, pl.ds(0, 8 * len(AG_S) - (0 in AG_S))], sem.at[it, 6])
            return 0

        lax.fori_loop(0, ITERS, help_out, 0)
        wait_for(kept.at[0], pair_sem.at[4])
        wait_for(ahead.at[0], pair_sem.at[7])
        wait_for_last_gradient(ITERS - 1)
        wait_for(plane_sum, pair_sem.at[9])
        finish(ITERS - 1, step_scale(plane_sum[...]), 0)

    @pl.when(core == 1)
    def _():
        def line_peer(dz):
            to = lax.rem(z + dz, 8)
            return {"feat": (to // 2) * 2 + 1, "tok": y * 8 + lax.rem(to, 2) * 4 + x}

        momentum = momentum_terms(ITERS)
        factor = DIN ** (-0.5)
        product[...] = first_product()
        ahead[1] = kept[1]
        pl.semaphore_wait(barrier, TOK + FEAT // 2 - 1)
        copy_to(act.at[1], act.at[1], pair_sem.at[2], pair_sem.at[3], partner)
        wait_for(pair_in, pair_sem.at[1])
        product[...] += pair_in[...]

        def iteration(it, _):
            def s(i):
                return sem.at[it, i]

            own = product[...]
            part_out[it] = own.astype(jnp.bfloat16)
            for k in (2, 1, 3):
                copy_to(part_out.at[it], part_in.at[it, k - 1], s(0), s(1), {"feat": lax.rem(feat + 2 * k, FEAT)})

            @pl.when(it == ITERS - 1)
            def _():
                copy_to(ahead.at[0], ahead.at[0], pair_sem.at[6], pair_sem.at[7], partner)

            wait_for(part_in.at[it], s(1))
            for k in range(3):
                own = own + part_in[it, k].astype(jnp.float32)
            left = (factor * own - goal[...]).astype(jnp.bfloat16)
            for half in range(2):
                residual[it, half] = jnp.concatenate(
                    [left[g * 16 + half * 8 : g * 16 + half * 8 + 8] for g in range(4)], axis=0
                )
            copy_to(residual.at[it, 0], residual.at[it, 0], s(10), s(11), partner)

            @pl.when(it == 0)
            def _():
                wait_for(act.at[0], pair_sem.at[3])

            send_pieces(it)
            arrived[it, 1, tok] = pieces[it, 1, tok]

            @pl.when(it == 0)
            def _():
                wait_for(kept.at[0], pair_sem.at[5])
                ahead[0] = kept[0]

            def summed(half):
                total = arrived[it, half, 0].astype(jnp.float32)
                for p in range(1, TOK):
                    total = total + arrived[it, half, p].astype(jnp.float32)
                return total

            wait_for(arrived.at[it, 1, pl.ds(0, TOK - 1)], s(3))
            lower = summed(1)
            wait_for(arrived.at[it, 0], s(14))
            upper = summed(0)
            gathered[it, tok] = jnp.concatenate([upper, lower], axis=0).astype(jnp.bfloat16)
            copy_to(gathered.at[it, tok], gathered.at[it, tok], s(12), s(13), partner)
            square = upper * upper + lower * lower
            lanes = square[:, :128]
            for c in range(1, TILES):
                lanes = lanes + square[:, c * 128 : c * 128 + 128]

            def spread(squares, slot, value, send, recv, devices):
                squares[it, slot] = value
                for device in devices:
                    copy_to(squares.at[it, slot], squares.at[it, slot], send, recv, device)

            def collected(squares, recv, number):
                wait_for(squares.at[it, pl.ds(0, number - 1)], recv)
                sums = [squares[it, p] for p in range(number)]
                while len(sums) > 1:
                    sums = [a + b for a, b in zip(sums[::2], sums[1::2])]
                return sums[0]

            spread(
                line_squares, z, jnp.sum(lanes, axis=0, keepdims=True), s(4), s(5),
                [line_peer(dz) for dz in LINE_PEERS],
            )
            send_gradient(it, AG_N)
            spread(
                plane_squares, y * 4 + x, collected(line_squares, s(5), 8), s(8), s(9),
                [{"tok": token_peer((dy, 0, dx))} for dy, dx in PLANE_PEERS],
            )
            plane_sum[...] = collected(plane_squares, s(9), 16)

            @pl.when(it == ITERS - 1)
            def _():
                copy_to(plane_sum, plane_sum, pair_sem.at[8], pair_sem.at[9], partner)

            scale = step_scale(plane_sum[...])
            m = jnp.float32(momentum[0])
            for i in range(1, ITERS):
                m = jnp.where(it == i, jnp.float32(momentum[i]), m)
            @pl.when(it < ITERS - 1)
            def _():
                wait_for(gathered.at[it, pl.ds(0, TOK - 1)], s(7))
                total = None
                for block in range(2):
                    for chunk in range(7):
                        low = []
                        for r in range(4):
                            line = []
                            for t in range(chunk * 4, chunk * 4 + 4):
                                rows, columns, shrunk = shrunk_tile(it, scale, block, r, t)
                                advance = shrunk + m * (shrunk - kept[block, rows, columns])
                                kept[block, rows, columns] = shrunk
                                ahead[block, rows, columns] = advance
                                line.append(advance.astype(jnp.bfloat16))
                            low.append(jnp.concatenate(line, axis=1))
                        part = lax.dot_general(
                            jnp.concatenate(low, axis=0), act[block, :, chunk * 512 : chunk * 512 + 512],
                            contract_last, preferred_element_type=jnp.float32,
                        )
                        total = part if total is None else total + part
                product[...] = total

            @pl.when(it == ITERS - 1)
            def _():
                wait_for_last_gradient(it)
                finish(it, scale, 1)
                wait_for(ahead.at[0], pair_sem.at[6])
                wait_for(plane_sum, pair_sem.at[8])

            wait_for(part_in.at[it], s(0))
            wait_for(pieces.at[it, 1, pl.ds(0, TOK - 1)], s(2))
            wait_for(line_squares.at[it, pl.ds(0, 7)], s(4))
            wait_for(gathered.at[it, pl.ds(0, 8 * len(AG_N) - (0 in AG_N))], s(6))
            wait_for(residual.at[it, 0], s(10))
            wait_for(gathered.at[it, tok], s(12))
            wait_for(plane_squares.at[it, pl.ds(0, 15)], s(8))
            return 0

        lax.fori_loop(0, ITERS, iteration, 0)
        wait_for(act.at[1], pair_sem.at[2])


def shards(activations, dense_rows, targets):
    bf16, f32 = jnp.bfloat16, jnp.float32
    half_buffer = pltpu.VMEM((ITERS, 2, TOK, PIECE_ROWS // 2, PIECE_COLS), bf16)
    piece_buffer = pltpu.VMEM((ITERS, TOK, PIECE_ROWS, PIECE_COLS), bf16)
    return pl.pallas_call(
        kernel,
        out_shape=pltpu.VMEM((ROWS, COLS), f32),
        in_specs=[pl.BlockSpec(memory_space=pltpu.HBM)] * 3,
        out_specs=pl.BlockSpec(memory_space=pltpu.VMEM),
        scratch_shapes=[
            pltpu.VMEM((2, TOKENS, COLS), bf16),
            pltpu.VMEM((ROWS, TOKENS), f32),
            pltpu.VMEM((2, ROWS, COLS), f32),
            pltpu.VMEM((2, ROWS, COLS), f32),
            pltpu.VMEM((ROWS, TOKENS), f32),
            pltpu.VMEM((ROWS, TOKENS), f32),
            pltpu.VMEM((ROWS, TOKENS), f32),
            pltpu.VMEM((ITERS, ROWS, TOKENS), bf16),
            pltpu.VMEM((ITERS, 3, ROWS, TOKENS), bf16),
            pltpu.VMEM((ITERS, 2, ROWS // 2, TOKENS), bf16),
            half_buffer,
            half_buffer,
            piece_buffer,
            pltpu.VMEM((ITERS, 8, 1, 128), f32),
            pltpu.VMEM((ITERS, 16, 1, 128), f32),
            pltpu.VMEM((1, 128), f32),
            pltpu.SemaphoreType.DMA((3,)),
            pltpu.SemaphoreType.DMA((10,)),
            pltpu.SemaphoreType.DMA((ITERS, 15)),
        ],
        compiler_params=pltpu.CompilerParams(collective_id=0, has_side_effects=True),
    )(activations, dense_rows, targets.T)


def solution(mesh):
    in_specs = (P("tok", "feat"), P(None, "feat"), P("tok", None))
    out_specs = P(None, "feat")
    return jax.shard_map(shards, mesh=mesh, in_specs=in_specs, out_specs=out_specs, check_vma=False)
```

```python
import math

import jax
import jax.numpy as jnp
from jax import lax
from jax.experimental import pallas as pl
from jax.experimental.pallas import tpu as pltpu
from jax.sharding import PartitionSpec as P

DIN = 28672
ROWS = 64
ITERS = 4

step_size = 0.25
threshold = 0.2
epsilon = 1e-06

MESH = pl.DeviceIdType.MESH
FEAT = 8
TOK = 32
TOKENS = 256
COLS = DIN // FEAT
PIECE_ROWS = 16
PIECE_COLS = COLS // 4
TILES = PIECE_COLS // 128


def momentum_terms(iterations):
    values = []
    current = 1.0
    for _ in range(iterations):
        upcoming = (1.0 + math.sqrt(1.0 + 4.0 * current * current)) / 2.0
        values.append((current - 1.0) / upcoming)
        current = upcoming
    return values


def ring(offset, size):
    return min(offset, size - offset)


TOKEN_PEERS = sorted(
    [(dy, dz, dx) for dy in range(4) for dz in range(2) for dx in range(4) if (dy, dz, dx) != (0, 0, 0)],
    key=lambda o: -(ring(o[0], 4) + o[1] + ring(o[2], 4)),
)
LINE_PEERS = sorted(range(1, 8), key=lambda o: -ring(o, 8))
PLANE_PEERS = sorted(
    [(dy, dx) for dy in range(4) for dx in range(4) if (dy, dx) != (0, 0)],
    key=lambda o: -(ring(o[0], 4) + ring(o[1], 4)),
)


COLUMN_PEERS = sorted([(dz, dx) for dz in range(2) for dx in range(4)], key=lambda o: -(o[0] + ring(o[1], 4)))


def kernel(
    act_hbm, dense_hbm, targets_hbm, weights,
    act, goal, kept, ahead, pair_out, pair_in, product, part_out, part_in, residual,
    pieces, arrived, gathered, line_squares, plane_squares, plane_sum,
    load_sem, pair_sem, sem,
):
    feat = lax.axis_index("feat")
    tok = lax.axis_index("tok")
    core = lax.rem(feat, 2)
    y, z_lo, x = tok // 8, lax.rem(tok // 4, 2), lax.rem(tok, 4)
    z = (feat // 2) * 2 + z_lo
    partner = {"feat": feat + 1 - 2 * core}

    def token_peer(offset):
        dy, dz, dx = offset
        return lax.rem(y + dy, 4) * 8 + lax.rem(z_lo + dz, 2) * 4 + lax.rem(x + dx, 4)

    barrier = pltpu.get_barrier_semaphore()

    @pl.when(core == 1)
    def _():
        for offset in TOKEN_PEERS:
            pl.semaphore_signal(barrier, inc=1, device_id={"tok": token_peer(offset)}, device_id_type=MESH)
        for k in (2, 1, 3):
            pl.semaphore_signal(
                barrier, inc=1, device_id={"feat": lax.rem(feat + 2 * k, FEAT)}, device_id_type=MESH
            )

    pl.semaphore_signal(barrier, inc=1, device_id=partner, device_id_type=MESH)
    load_dense = pltpu.make_async_copy(dense_hbm, kept.at[core], load_sem.at[0])
    load_act = pltpu.make_async_copy(act_hbm, act.at[core], load_sem.at[1])
    load_goal = pltpu.make_async_copy(targets_hbm, goal, load_sem.at[2])
    load_dense.start()
    load_act.start()
    load_goal.start()

    def copy_to(src, dst, send, recv, device):
        pltpu.make_async_remote_copy(
            src_ref=src, dst_ref=dst, send_sem=send, recv_sem=recv, device_id=device, device_id_type=MESH
        ).start()

    def wait_for(ref, semaphore):
        pltpu.make_async_copy(ref, ref, semaphore).wait()

    contract_last = (((1,), (1,)), ((), ()))

    def first_product():
        load_dense.wait()
        load_act.wait()
        load_goal.wait()
        return lax.dot_general(
            kept[core].astype(jnp.bfloat16), act[core], contract_last, preferred_element_type=jnp.float32
        )

    def send_pieces(it):
        residuals = residual[it, core]
        arrival = sem.at[it, 14 - 11 * core]
        for dz, dx in COLUMN_PEERS:
            block, cx = lax.rem(z_lo + dz, 2), lax.rem(x + dx, 4)
            columns = pl.ds(pl.multiple_of(cx * PIECE_COLS, 128), PIECE_COLS)
            part = jnp.dot(residuals, act[block, :, columns], preferred_element_type=jnp.float32)
            for g in range(4):
                pieces[it, core, g * 8 + block * 4 + cx] = part[g * 8 : g * 8 + 8].astype(jnp.bfloat16)
            for dy in (2, 1, 3, 0):
                if (dy, dz, dx) != (0, 0, 0):
                    to = token_peer((dy, dz, dx))
                    copy_to(
                        pieces.at[it, core, to], arrived.at[it, core, tok], sem.at[it, 2], arrival,
                        {"feat": feat + 1 - core, "tok": to},
                    )

    def send_gradient(it):
        target = feat - core + jnp.where(it == ITERS - 1, z_lo, 1)
        half = gathered.at[it, core, tok]
        for offset in TOKEN_PEERS:
            copy_to(
                half, half, sem.at[it, 6], sem.at[it, 15 - 8 * core], {"feat": target, "tok": token_peer(offset)}
            )

    def wait_for_last_gradient(it):
        @pl.when(z_lo == core)
        def _():
            wait_for(gathered.at[it, 1, pl.ds(0, TOK // 2 - 1)], sem.at[it, 7])
            wait_for(gathered.at[it, 0, pl.ds(0, TOK // 2 - 1)], sem.at[it, 15])

        @pl.when(z_lo != core)
        def _():
            wait_for(gathered.at[it, 1, pl.ds(0, TOK // 2)], sem.at[it, 7])
            wait_for(gathered.at[it, 0, pl.ds(0, TOK // 2)], sem.at[it, 15])

    def step_scale(lanes):
        total_square = jnp.sum(lanes, axis=1, keepdims=True)
        return step_size * lax.rsqrt(total_square / (ROWS * DIN) + epsilon)

    def shrunk_tile(it, scale, block, r, t):
        rows, columns = slice(r * 16, r * 16 + 16), slice(t * 128, t * 128 + 128)
        inner = slice((t % TILES) * 128, (t % TILES) * 128 + 128)
        gradient = jnp.concatenate(
            [gathered[it, half, r * 8 + block * 4 + t // TILES, :, inner].astype(jnp.float32) for half in range(2)],
            axis=0,
        )
        moved = ahead[block, rows, columns] - scale * gradient
        return rows, columns, moved - jnp.clip(moved, -threshold, threshold)

    def finish(it, scale, block):
        for t in range(4 * TILES):
            for r in range(4):
                rows, columns, shrunk = shrunk_tile(it, scale, block, r, t)
                weights[rows, columns] = shrunk

    @pl.when(core == 0)
    def _():
        pair_out[...] = first_product()
        pl.semaphore_wait(barrier, 1)
        copy_to(pair_out, pair_in, pair_sem.at[0], pair_sem.at[1], partner)
        copy_to(act.at[0], act.at[0], pair_sem.at[2], pair_sem.at[3], partner)
        copy_to(kept.at[0], kept.at[0], pair_sem.at[4], pair_sem.at[5], partner)
        wait_for(pair_out, pair_sem.at[0])
        wait_for(act.at[0], pair_sem.at[2])
        wait_for(act.at[1], pair_sem.at[3])

        def help_out(it, _):
            wait_for(residual.at[it, 0], sem.at[it, 11])
            send_pieces(it)
            copy_to(pieces.at[it, 0, tok], arrived.at[it, 0, tok], sem.at[it, 2], sem.at[it, 14], partner)
            wait_for(gathered.at[it, 0, tok], sem.at[it, 13])
            send_gradient(it)
            wait_for(gathered.at[it, 1, tok], sem.at[it, 16])
            wait_for(pieces.at[it, 0], sem.at[it, 2])
            wait_for(gathered.at[it, 0, pl.ds(0, TOK - 1)], sem.at[it, 6])
            return 0

        lax.fori_loop(0, ITERS, help_out, 0)
        wait_for(kept.at[0], pair_sem.at[4])
        wait_for(ahead.at[0], pair_sem.at[7])
        wait_for_last_gradient(ITERS - 1)
        wait_for(plane_sum, pair_sem.at[9])
        finish(ITERS - 1, step_scale(plane_sum[...]), 0)

    @pl.when(core == 1)
    def _():
        def line_peer(dz):
            to = lax.rem(z + dz, 8)
            return {"feat": (to // 2) * 2 + 1, "tok": y * 8 + lax.rem(to, 2) * 4 + x}

        momentum = momentum_terms(ITERS)
        factor = DIN ** (-0.5)
        product[...] = first_product()
        ahead[1] = kept[1]
        pl.semaphore_wait(barrier, TOK + FEAT // 2 - 1)
        copy_to(act.at[1], act.at[1], pair_sem.at[2], pair_sem.at[3], partner)
        wait_for(pair_in, pair_sem.at[1])
        product[...] += pair_in[...]

        def iteration(it, _):
            def s(i):
                return sem.at[it, i]

            own = product[...]
            part_out[it] = own.astype(jnp.bfloat16)
            for k in (2, 1, 3):
                copy_to(part_out.at[it], part_in.at[it, k - 1], s(0), s(1), {"feat": lax.rem(feat + 2 * k, FEAT)})

            @pl.when(it == ITERS - 1)
            def _():
                copy_to(ahead.at[0], ahead.at[0], pair_sem.at[6], pair_sem.at[7], partner)

            wait_for(part_in.at[it], s(1))
            for k in range(3):
                own = own + part_in[it, k].astype(jnp.float32)
            left = (factor * own - goal[...]).astype(jnp.bfloat16)
            for half in range(2):
                residual[it, half] = jnp.concatenate(
                    [left[g * 16 + half * 8 : g * 16 + half * 8 + 8] for g in range(4)], axis=0
                )
            copy_to(residual.at[it, 0], residual.at[it, 0], s(10), s(11), partner)

            @pl.when(it == 0)
            def _():
                wait_for(act.at[0], pair_sem.at[3])

            send_pieces(it)
            arrived[it, 1, tok] = pieces[it, 1, tok]

            @pl.when(it == 0)
            def _():
                wait_for(kept.at[0], pair_sem.at[5])
                ahead[0] = kept[0]

            def summed(half):
                total = arrived[it, half, 0].astype(jnp.float32)
                for p in range(1, TOK):
                    total = total + arrived[it, half, p].astype(jnp.float32)
                return total

            wait_for(arrived.at[it, 1, pl.ds(0, TOK - 1)], s(3))
            lower = summed(1)
            gathered[it, 1, tok] = lower.astype(jnp.bfloat16)
            send_gradient(it)
            copy_to(gathered.at[it, 1, tok], gathered.at[it, 1, tok], s(17), s(16), partner)
            wait_for(arrived.at[it, 0], s(14))
            upper = summed(0)
            gathered[it, 0, tok] = upper.astype(jnp.bfloat16)
            copy_to(gathered.at[it, 0, tok], gathered.at[it, 0, tok], s(12), s(13), partner)
            square = upper * upper + lower * lower
            lanes = square[:, :128]
            for c in range(1, TILES):
                lanes = lanes + square[:, c * 128 : c * 128 + 128]

            def spread(squares, slot, value, send, recv, devices):
                squares[it, slot] = value
                for device in devices:
                    copy_to(squares.at[it, slot], squares.at[it, slot], send, recv, device)

            def collected(squares, recv, number):
                wait_for(squares.at[it, pl.ds(0, number - 1)], recv)
                sums = [squares[it, p] for p in range(number)]
                while len(sums) > 1:
                    sums = [a + b for a, b in zip(sums[::2], sums[1::2])]
                return sums[0]

            spread(
                line_squares, z, jnp.sum(lanes, axis=0, keepdims=True), s(4), s(5),
                [line_peer(dz) for dz in LINE_PEERS],
            )
            spread(
                plane_squares, y * 4 + x, collected(line_squares, s(5), 8), s(8), s(9),
                [{"tok": token_peer((dy, 0, dx))} for dy, dx in PLANE_PEERS],
            )
            plane_sum[...] = collected(plane_squares, s(9), 16)

            @pl.when(it == ITERS - 1)
            def _():
                copy_to(plane_sum, plane_sum, pair_sem.at[8], pair_sem.at[9], partner)

            scale = step_scale(plane_sum[...])
            m = jnp.float32(momentum[0])
            for i in range(1, ITERS):
                m = jnp.where(it == i, jnp.float32(momentum[i]), m)
            @pl.when(it < ITERS - 1)
            def _():
                wait_for(gathered.at[it, 1, pl.ds(0, TOK - 1)], s(7))
                wait_for(gathered.at[it, 0, pl.ds(0, TOK - 1)], s(15))
                total = None
                for block in range(2):
                    for chunk in range(7):
                        low = []
                        for r in range(4):
                            line = []
                            for t in range(chunk * 4, chunk * 4 + 4):
                                rows, columns, shrunk = shrunk_tile(it, scale, block, r, t)
                                advance = shrunk + m * (shrunk - kept[block, rows, columns])
                                kept[block, rows, columns] = shrunk
                                ahead[block, rows, columns] = advance
                                line.append(advance.astype(jnp.bfloat16))
                            low.append(jnp.concatenate(line, axis=1))
                        part = lax.dot_general(
                            jnp.concatenate(low, axis=0), act[block, :, chunk * 512 : chunk * 512 + 512],
                            contract_last, preferred_element_type=jnp.float32,
                        )
                        total = part if total is None else total + part
                product[...] = total

            @pl.when(it == ITERS - 1)
            def _():
                wait_for_last_gradient(it)
                finish(it, scale, 1)
                wait_for(ahead.at[0], pair_sem.at[6])
                wait_for(plane_sum, pair_sem.at[8])

            wait_for(part_in.at[it], s(0))
            wait_for(pieces.at[it, 1, pl.ds(0, TOK - 1)], s(2))
            wait_for(line_squares.at[it, pl.ds(0, 7)], s(4))
            wait_for(gathered.at[it, 1, pl.ds(0, TOK - 1)], s(6))
            wait_for(gathered.at[it, 1, tok], s(17))
            wait_for(residual.at[it, 0], s(10))
            wait_for(gathered.at[it, 0, tok], s(12))
            wait_for(plane_squares.at[it, pl.ds(0, 15)], s(8))
            return 0

        lax.fori_loop(0, ITERS, iteration, 0)
        wait_for(act.at[1], pair_sem.at[2])


def shards(activations, dense_rows, targets):
    bf16, f32 = jnp.bfloat16, jnp.float32
    half_buffer = pltpu.VMEM((ITERS, 2, TOK, PIECE_ROWS // 2, PIECE_COLS), bf16)
    return pl.pallas_call(
        kernel,
        out_shape=pltpu.VMEM((ROWS, COLS), f32),
        in_specs=[pl.BlockSpec(memory_space=pltpu.HBM)] * 3,
        out_specs=pl.BlockSpec(memory_space=pltpu.VMEM),
        scratch_shapes=[
            pltpu.VMEM((2, TOKENS, COLS), bf16),
            pltpu.VMEM((ROWS, TOKENS), f32),
            pltpu.VMEM((2, ROWS, COLS), f32),
            pltpu.VMEM((2, ROWS, COLS), f32),
            pltpu.VMEM((ROWS, TOKENS), f32),
            pltpu.VMEM((ROWS, TOKENS), f32),
            pltpu.VMEM((ROWS, TOKENS), f32),
            pltpu.VMEM((ITERS, ROWS, TOKENS), bf16),
            pltpu.VMEM((ITERS, 3, ROWS, TOKENS), bf16),
            pltpu.VMEM((ITERS, 2, ROWS // 2, TOKENS), bf16),
            half_buffer,
            half_buffer,
            half_buffer,
            pltpu.VMEM((ITERS, 8, 1, 128), f32),
            pltpu.VMEM((ITERS, 16, 1, 128), f32),
            pltpu.VMEM((1, 128), f32),
            pltpu.SemaphoreType.DMA((3,)),
            pltpu.SemaphoreType.DMA((10,)),
            pltpu.SemaphoreType.DMA((ITERS, 18)),
        ],
        compiler_params=pltpu.CompilerParams(collective_id=0, has_side_effects=True),
    )(activations, dense_rows, targets.T)


def solution(mesh):
    in_specs = (P("tok", "feat"), P(None, "feat"), P("tok", None))
    out_specs = P(None, "feat")
    return jax.shard_map(shards, mesh=mesh, in_specs=in_specs, out_specs=out_specs, check_vma=False)
```
